512 devices in a mesh: dp: 32 (over z_lo, y, core), blk: 16 (over x, z_hi).
Axes of the slice: x: 4, y: 4, z: 16 (z_hi: 4, z_lo: 4; z = z_hi * 4 + z_lo), core: 2. Of those that a mesh axis runs over, the one named last changes fastest.
Arguments:
- block_input_rows: bfloat16 [9216, 16384], P('dp', 'blk'), may hold values from -6 to 6
- up_loss_gradient: bfloat16 [9216, 53248], P('dp', 'blk'), may hold values from -6 to 6
- down_projection_input: bfloat16 [9216, 53248], P('dp', 'blk'), may hold values from -6 to 6
- output_loss_gradient: bfloat16 [9216, 16384], P('dp', 'blk'), may hold values from -6 to 6
- model_side_factors: bfloat16 [2, 32, 16384], P(None, 'dp', 'blk'), may hold values from -0.046875 to 0.046875
- hidden_side_factors: bfloat16 [2, 32, 53248], P(None, 'dp', 'blk'), may hold values from -0.02734375 to 0.02734375
- example_index_rows: int32 [32, 288], P('dp'), may hold values from 0 to 7, never falling along the last dimension, each value on 1 to 72 neighbouring positions
- clipping_threshold: int32 [1], replicated, may hold values from 0 to 7
- model_side_noise: float32 [2, 32, 16384], P(None, 'dp', 'blk'), may hold values from -6 to 6
- hidden_side_noise: float32 [2, 32, 53248], P(None, 'dp', 'blk'), may hold values from -6 to 6
Outputs:
- update_model: float32 [2, 32, 16384], P(None, 'dp', 'blk')
- update_hidden: float32 [2, 32, 53248], P(None, 'dp', 'blk')
The draws below stay inside these ranges and needn't reach their ends.
Inputs may be any that keep to these rules, and one draw needn't show every extreme that they name: `example_index_rows`: along each row the ids never fall, every id 0 to 7 occurs, and an example has at most 72 tokens, some example exactly that many.
All inputs are finite; a program needn't handle non-finite values.
Results may differ from the reference program's by a relative error of at most 0.0003.
Values may be sent and summed in bfloat16 or wider, within the bound.
A program may use at most 64 MiB of HBM per device.

```python
import math
import jax
import jax.numpy as jnp
import numpy as np
from jax import lax

MODEL_WIDTH = 16384
HIDDEN_UNITS = 53248
ADAPTER_RANK = 32
EX = 8
TOK_DEV = 288
TOKENS = 9216
N_DP = 32


def shard_levels(stream_key, dims, shards, low, high):
    def one(dim, parts):
        draws = jax.random.uniform(jax.random.fold_in(jax.random.fold_in(stream_key, 6), dim), (parts,), jnp.float32, low / len(shards), high / len(shards))
        return jnp.repeat(jnp.exp(draws), dims[dim] // parts).reshape((-1,) + (1,) * (len(dims) - dim - 1))

    gain = one(*shards[0])
    for cut in shards[1:]:
        gain = gain * one(*cut)
    return gain


def split_up(number_of, total, most, slope):
    loads = [(1 << 20) // math.isqrt(grade ** slope) + 1 for grade in range(2, number_of + 1)]
    spare, given = total - most - (number_of - 1), [1] * (number_of - 1)
    while spare > 0:
        movable = [i for i in range(number_of - 1) if given[i] < most]
        pool, budget = sum([loads[i] for i in movable]), spare
        for i in movable:
            addition = min(most - given[i], max(1, budget * loads[i] // pool), spare)
            given[i] = given[i] + addition
            spare = spare - addition
    return np.array([most] + given)


def ragged_sizes(rng, count, total, most, slope):
    if count == 2:
        one = jax.random.randint(rng, (), max(1, total - most), min(most, total - 1) + 1)
        return jnp.stack([one, total - one])
    sizes = jnp.asarray(split_up(count, total, most, slope), jnp.int32)
    twos = (count - 1) // 2
    donor, sink = sizes[1:1 + 2 * twos:2], sizes[2:2 + 2 * twos:2]
    room = jnp.minimum(donor - 1, most - sink)
    shifted = jax.random.randint(jax.random.fold_in(rng, 1), (twos,), 0, 1 << 20) % (room + 1)
    sizes = sizes.at[1:1 + 2 * twos:2].set(donor - shifted).at[2:2 + 2 * twos:2].set(sink + shifted)
    return sizes[jax.random.permutation(jax.random.fold_in(rng, 2), count)]


def scatter_about(key, dims, spread, bound, shards=(), held_as=jnp.bfloat16):
    entries = jax.random.normal(key, dims, jnp.float32) * spread
    if len(shards) > 0:
        entries = shard_levels(key, dims, shards, -0.22, 0.18) * entries
    return jnp.clip(entries, min=-bound, max=bound).astype(held_as)


def setup_inputs(seed: int = 0) -> dict:
    splits = jax.random.split(jax.random.key(seed), 11)
    return {
        "block_input_rows": scatter_about(splits[0], (TOKENS, MODEL_WIDTH), 1.0, 6.0, ((0, 32), (1, 16))),
        "up_loss_gradient": scatter_about(splits[1], (TOKENS, HIDDEN_UNITS), 1.0, 6.0, ((0, 32), (1, 16))),
        "down_projection_input": scatter_about(splits[2], (TOKENS, HIDDEN_UNITS), 1.0, 6.0, ((0, 32), (1, 16))),
        "output_loss_gradient": scatter_about(splits[3], (TOKENS, MODEL_WIDTH), 1.0, 6.0, ((0, 32), (1, 16))),
        "model_side_factors": scatter_about(splits[4], (2, ADAPTER_RANK, MODEL_WIDTH), MODEL_WIDTH ** -0.5, 0.046875, ((1, 32), (2, 16))),
        "hidden_side_factors": scatter_about(splits[5], (2, ADAPTER_RANK, HIDDEN_UNITS), HIDDEN_UNITS ** -0.5, 0.02734375, ((1, 32), (2, 16))),
        "example_index_rows": jax.vmap(lambda own: jnp.searchsorted(jnp.cumsum(ragged_sizes(own, EX, TOK_DEV, TOK_DEV // 4, 2)), jnp.arange(TOK_DEV), side="right"))(jax.random.split(splits[6], N_DP)).reshape((N_DP, TOK_DEV)).astype(jnp.int32),
        "clipping_threshold": jax.random.randint(splits[7], (1,), 0, 8).astype(jnp.int32),
        "model_side_noise": scatter_about(splits[8], (2, ADAPTER_RANK, MODEL_WIDTH), 1.0, 6.0, ((1, 32), (2, 16)), jnp.float32),
        "hidden_side_noise": scatter_about(splits[9], (2, ADAPTER_RANK, HIDDEN_UNITS), 1.0, 6.0, ((1, 32), (2, 16)), jnp.float32),
    }


def projected_pairs(input_activation, up_gradient, hidden_activation, output_gradient, model_side_factors, hidden_side_factors):
    input_projected = jnp.dot(input_activation, model_side_factors[0].T, preferred_element_type=jnp.float32)
    up_backward = jnp.dot(up_gradient, hidden_side_factors[0].T, preferred_element_type=jnp.float32)
    hidden_projected = jnp.dot(hidden_activation, hidden_side_factors[1].T, preferred_element_type=jnp.float32)
    down_backward = jnp.dot(output_gradient, model_side_factors[1].T, preferred_element_type=jnp.float32)
    return (input_projected, up_backward, hidden_projected, down_backward)

def membership(doc_ids):
    return (doc_ids[None, :] == jnp.arange(EX, dtype=jnp.int32)[:, None]).astype(jnp.float32)

def highest_dot(narrow, broad):
    return jnp.dot(narrow, broad.astype(jnp.float32), precision=lax.Precision.HIGHEST)

def reference(block_input_rows, up_loss_gradient, down_projection_input, output_loss_gradient, model_side_factors, hidden_side_factors, example_index_rows, clipping_threshold, model_side_noise, hidden_side_noise):
    stacked = (block_input_rows.reshape(N_DP, TOK_DEV, MODEL_WIDTH), up_loss_gradient.reshape(N_DP, TOK_DEV, HIDDEN_UNITS), down_projection_input.reshape(N_DP, TOK_DEV, HIDDEN_UNITS), output_loss_gradient.reshape(N_DP, TOK_DEV, MODEL_WIDTH), example_index_rows)

    def group_norms(slices):
        input_activation, up_gradient, hidden_activation, output_gradient, doc_ids = slices
        input_projected, up_backward, hidden_projected, down_backward = projected_pairs(input_activation, up_gradient, hidden_activation, output_gradient, model_side_factors, hidden_side_factors)
        member = membership(doc_ids)
        total_sq = jnp.zeros((EX,), jnp.float32)
        for narrow, broad in ((up_backward, input_activation), (hidden_projected, output_gradient), (input_projected, up_gradient), (down_backward, hidden_activation)):
            weighted = member[:, :, None] * narrow[None, :, :]
            per_ex = jnp.einsum('etr,tf->erf', weighted, broad.astype(jnp.float32), precision=lax.Precision.HIGHEST)
            total_sq = total_sq + lax.optimization_barrier(jnp.sum(per_ex * per_ex, axis=(1, 2)))
        return total_sq
    norm_sq = lax.map(group_norms, stacked)
    grand_total = jnp.sum(norm_sq)
    root_mean = jnp.sqrt(grand_total / (N_DP * EX) + 1e-06)
    clip_bound = (0.5 + 0.125 * clipping_threshold[0].astype(jnp.float32)) * root_mean
    factors = jnp.minimum(1.0, clip_bound * lax.rsqrt(norm_sq + 1e-06))

    def group_grads(running, slices):
        input_activation, up_gradient, hidden_activation, output_gradient, doc_ids, factor_row = slices
        input_projected, up_backward, hidden_projected, down_backward = projected_pairs(input_activation, up_gradient, hidden_activation, output_gradient, model_side_factors, hidden_side_factors)
        member = membership(doc_ids)
        tok_factor = jnp.dot(factor_row, member, precision=lax.Precision.HIGHEST)[:, None]
        model_part = jnp.stack([highest_dot((tok_factor * up_backward).T, input_activation), highest_dot((tok_factor * hidden_projected).T, output_gradient)])
        hidden_part = jnp.stack([highest_dot((tok_factor * input_projected).T, up_gradient), highest_dot((tok_factor * down_backward).T, hidden_activation)])
        return ((running[0] + model_part, running[1] + hidden_part), None)
    start = (jnp.zeros((2, ADAPTER_RANK, MODEL_WIDTH), jnp.float32), jnp.zeros((2, ADAPTER_RANK, HIDDEN_UNITS), jnp.float32))
    (sum_model, sum_hidden), unused = lax.scan(group_grads, start, stacked + (factors,))
    rescale = jnp.sqrt(jnp.float32(2 * ADAPTER_RANK * (MODEL_WIDTH + HIDDEN_UNITS)) / (N_DP * EX)) / clip_bound
    return (sum_model * rescale + model_side_noise, sum_hidden * rescale + hidden_side_noise)
```

```python
import functools
import math

import jax
import jax.numpy as jnp
from jax import lax
from jax.experimental import pallas as pl
from jax.experimental.pallas import tpu as pltpu
from jax.sharding import PartitionSpec as P

EX = 8
LANES = 128
SLOT = 32
DP_AXES = {32: (4, 4, 2), 4: (2, 1, 2), 8: (2, 2, 2)}
BLK_AXES = {16: (4, 4), 4: (2, 2), 2: (1, 2)}
PAIR = (1, 0, 3, 2)
F32 = jnp.float32
BF16 = jnp.bfloat16


def nt(a, b):
    return lax.dot_general(a, b, (((1,), (1,)), ((), ())), preferred_element_type=F32)


def nn(a, b):
    return lax.dot_general(a, b, (((1,), (0,)), ((), ())), preferred_element_type=F32)


def split(a):
    high = a.astype(BF16)
    return high, (a - high.astype(F32)).astype(BF16)


def remote(src, dst, send, recv, **where):
    return pltpu.make_async_remote_copy(
        src_ref=src,
        dst_ref=dst,
        send_sem=send,
        recv_sem=recv,
        device_id=where,
        device_id_type=pl.DeviceIdType.MESH,
    )


def kernel(
    cfg,
    thr_ref,
    ids_ref,
    row_ref,
    a0,
    a1,
    a2,
    a3,
    out_ref,
    wide,
    rows_in,
    rows_f32,
    factors,
    gram_hi,
    gram_lo,
    part,
    part_in,
    quarter,
    quarter_in,
    proj,
    plane,
    ring,
    grads,
    pair_in,
    pair_sum,
    y_in,
    z_out,
    z_in,
    load_sem,
    row_send,
    row_recv,
    part_send,
    part_recv,
    quarter_send,
    quarter_recv,
    proj_send,
    proj_recv,
    plane_send,
    plane_recv,
    ring_send,
    ring_recv,
    pair_send,
    pair_recv,
    y_send,
    y_recv,
    z_send,
    z_recv,
):
    NZL, NY, NC, NX, NZH, widths, block = cfg
    tokens = wide.shape[0]
    ranks = NZL * NY * NC
    dp, blk = lax.axis_index("dp"), lax.axis_index("blk")
    zl, y, c = dp // (NY * NC), (dp // NC) % NY, dp % NC
    x, zh = blk // NZH, blk % NZH
    nz, npl = NZL * NZH, NX * NY * NC
    zz = zh * NZL + zl
    pp = (x * NY + y) * NC + c

    def dp_of(z_, y_, c_):
        return (z_ * NY + y_) * NC + c_

    def slot_of(z_, y_, c_):
        return (c_ * NZL + z_) * NY + y_

    def plane_where(k):
        q = (pp + k) % npl
        x_, y_, c_ = q // (NY * NC), (q // NC) % NY, q % NC
        return {"dp": dp_of(zl, y_, c_), "blk": x_ * NZH + zh}

    def ring_where(k):
        q = (zz + k) % nz
        return {"dp": dp_of(q % NZL, y, c), "blk": x * NZH + q // NZL}

    offsets = [sum(widths[:i]) for i in range(4)]
    loads = []
    for i, ref in enumerate((a0, a1, a2, a3)):
        copy = pltpu.make_async_copy(
            ref, wide.at[:, pl.ds(offsets[i], widths[i])], load_sem.at[i]
        )
        copy.start()
        loads.append(copy)

    barrier = pltpu.get_barrier_semaphore()

    def greet_plane(k, carry):
        pl.semaphore_signal(
            barrier, inc=1, device_id=plane_where(k), device_id_type=pl.DeviceIdType.MESH
        )
        return carry

    def greet_ring(k, carry):
        pl.semaphore_signal(
            barrier, inc=1, device_id=ring_where(k), device_id_type=pl.DeviceIdType.MESH
        )
        return carry

    lax.fori_loop(1, npl, greet_plane, 0)
    lax.fori_loop(1, nz, greet_ring, 0)

    half, reach = tokens // 2, 256
    member_t = (
        jnp.broadcast_to(ids_ref[...], (LANES, tokens))
        == lax.broadcasted_iota(jnp.int32, (LANES, tokens), 0)
    ).astype(F32).astype(BF16)
    eye = (
        lax.broadcasted_iota(jnp.int32, (tokens, tokens), 0)
        == lax.broadcasted_iota(jnp.int32, (tokens, tokens), 1)
    ).astype(F32).astype(BF16)
    member = nt(eye, member_t)
    member_b = member.astype(BF16)
    starts = (0, tokens - reach)
    factors[...] = jnp.zeros_like(factors)

    pl.semaphore_wait(barrier, npl - 1 + nz - 1)

    own = slot_of(zl, y, c)
    sends = []

    def row_copy(src, slot, where):
        copy = remote(src, rows_in.at[slot], row_send.at[len(sends)], row_recv.at[slot], dp=where)
        copy.start()
        sends.append(copy)

    def row_wait(slot):
        remote(
            rows_in.at[slot], rows_in.at[slot], row_send.at[0], row_recv.at[slot], dp=dp_of(zl, y, 1 - c)
        ).wait_recv()

    for k in range(1, NZL):
        row_copy(row_ref, own, dp_of((zl + k) % NZL, y, c))
    for j in range(1, NY):
        row_copy(row_ref, own, dp_of(zl, (y + j) % NY, c))
    row_copy(row_ref, own, dp_of(zl, y, 1 - c))

    for i in (0, 3, 1, 2):
        loads[i].wait()
        for b in range(2):
            same = nt(member_b[b * half : (b + 1) * half], member_b[starts[b] : starts[b] + reach])
            total = jnp.zeros((half, reach), F32)
            for k in range(0, widths[i], 256):
                n = min(256, widths[i] - k)
                at = offsets[i] + k
                total += nt(
                    wide[b * half : (b + 1) * half, at : at + n],
                    wide[starts[b] : starts[b] + reach, at : at + n],
                )
            high, low = split(jnp.where(same > 0.5, total, 0.0))
            gram_hi[i, b] = high
            gram_lo[i, b] = low

    for k in range(1, NZL):
        z_ = (zl + k) % NZL
        slot = slot_of(z_, y, c)
        row_wait(slot)
        for j in range(1, NY):
            row_copy(rows_in.at[slot], slot, dp_of(zl, (y + j) % NY, c))
        row_copy(rows_in.at[slot], slot, dp_of(zl, y, 1 - c))
    for k in range(NZL):
        for j in range(1, NY):
            slot = slot_of((zl + k) % NZL, (y + j) % NY, c)
            row_wait(slot)
            row_copy(rows_in.at[slot], slot, dp_of(zl, y, 1 - c))

    def widen(ref, slot):
        at = pl.multiple_of(slot * block, 8)
        rows_f32[pl.ds(at, block), :] = ref[...].astype(F32)[:block]

    widen(row_ref, own)
    for k in range(NZL):
        for j in range(NY):
            if k or j:
                slot = slot_of((zl + k) % NZL, (y + j) % NY, c)
                widen(rows_in.at[slot], slot)
    for k in range(NZL):
        for j in range(NY):
            slot = slot_of((zl + k) % NZL, (y + j) % NY, 1 - c)
            row_wait(slot)
            widen(rows_in.at[slot], slot)

    chunks = [w // LANES for w in widths]
    firsts = (0, chunks[0] + chunks[3], chunks[0] + chunks[3] + chunks[1], chunks[0])
    for i in range(4):
        for j in range(chunks[i]):
            picked = rows_f32[pl.ds(firsts[i] + j, ranks, stride=block), :]
            at = offsets[i] + j * LANES
            factors[SLOT * i : SLOT * i + ranks, at : at + LANES] = picked.astype(BF16)

    total = jnp.zeros((tokens, LANES), F32)
    for k in range(0, wide.shape[1], 256):
        n = min(256, wide.shape[1] - k)
        total += nt(wide[:, k : k + n], factors[:, k : k + n])
    part[...] = total.reshape(part.shape)

    copies = []
    for k in range(1, NX):
        x_ = (x + k) % NX
        copy = remote(
            part.at[x_], part_in.at[x], part_send.at[k], part_recv.at[k], blk=x_ * NZH + zh
        )
        copy.start()
        copies.append(copy)
    for copy in copies:
        copy.wait_recv()
    held = part[x]
    for k in range(1, NX):
        held += part_in[(x + k) % NX]
    quarter[...] = held
    sends += copies
    copies = []
    for k in range(1, NZH):
        copy = remote(
            quarter,
            quarter_in.at[zh],
            quarter_send.at[k],
            quarter_recv.at[k],
            blk=x * NZH + (zh + k) % NZH,
        )
        copy.start()
        copies.append(copy)
    for copy in copies:
        copy.wait_recv()
    for k in range(1, NZH):
        held += quarter_in[(zh + k) % NZH]
    proj[x] = held
    sends += copies
    copies = []
    for k in range(1, NX):
        copy = remote(
            proj.at[x], proj.at[x], proj_send.at[k], proj_recv.at[k], blk=((x + k) % NX) * NZH + zh
        )
        copy.start()
        copies.append(copy)
    for copy in copies:
        copy.wait_recv()
    sends += copies

    sums = proj[...].reshape(tokens, LANES)
    high, low = split(sums)
    both = jnp.concatenate([high, low], axis=1)
    lane = lax.broadcasted_iota(jnp.int32, (half, LANES), 1) // SLOT
    norm = jnp.zeros((1, LANES), F32)
    for b in range(2):
        mixed = jnp.zeros((half, LANES), F32)
        for i in range(4):
            first = nn(gram_hi[i, b], both[starts[b] : starts[b] + reach])
            second = nn(gram_lo[i, b], high[starts[b] : starts[b] + reach])
            term = first[:, :LANES] + first[:, LANES:] + second
            mixed = jnp.where(lane == PAIR[i], term, mixed)
        mine = sums[b * half : (b + 1) * half]
        each = jnp.sum(mixed * mine, axis=1, keepdims=True)
        norm += jnp.sum(member[b * half : (b + 1) * half] * each, axis=0, keepdims=True)

    plane[pp] = norm

    def plane_copy(k):
        return remote(plane.at[pp], plane.at[pp], plane_send, plane_recv, **plane_where(k))

    def plane_start(k, carry):
        plane_copy(k).start()
        return carry

    lax.fori_loop(1, npl, plane_start, 0)
    rest = plane.at[pl.ds(0, npl - 1)]
    remote(rest, rest, plane_send, plane_recv, **plane_where(1)).wait()
    everyone = jnp.sum(plane[...], axis=0)
    group = jnp.zeros((1, LANES), F32)
    for k in range(NX):
        group += plane[(k * NY + y) * NC + c]
    ring[zz] = jnp.concatenate([group, everyone], axis=0)

    def ring_start(k, carry):
        remote(ring.at[zz], ring.at[zz], ring_send, ring_recv, **ring_where(k)).start()
        return carry

    lax.fori_loop(1, nz, ring_start, 0)
    rest = ring.at[pl.ds(0, nz - 1)]
    remote(rest, rest, ring_send, ring_recv, **ring_where(1)).wait()
    everyone = jnp.sum(ring[...], axis=0)[1:2]
    group = jnp.zeros((1, LANES), F32)
    for k in range(NZH):
        group += ring[k * NZL + zl][0:1]
    grand_total = jnp.sum(everyone, axis=1, keepdims=True)
    root_mean = jnp.sqrt(jnp.maximum(grand_total, 0.0) / (ranks * EX) + 1e-06)
    clip = (0.5 + 0.125 * thr_ref[0].astype(F32)) * root_mean
    factor = jnp.minimum(1.0, clip * lax.rsqrt(jnp.maximum(group, 0.0) + 1e-06))
    entries = 2 * ranks * NX * NZH * (widths[0] + widths[1])
    rescale = math.sqrt(entries / (ranks * EX)) / clip
    weight = jnp.sum(member * (factor * rescale), axis=1, keepdims=True)

    high, low = split(weight * sums)
    eye = (
        lax.broadcasted_iota(jnp.int32, (LANES, LANES), 0)
        == lax.broadcasted_iota(jnp.int32, (LANES, LANES), 1)
    ).astype(F32).astype(BF16)
    high_t, low_t = nt(eye, high).astype(BF16), nt(eye, low).astype(BF16)
    for i in range(4):
        at = SLOT * PAIR[i]
        left = jnp.concatenate([high_t[at : at + SLOT], low_t[at : at + SLOT]], axis=0)
        for k in range(0, widths[i], 256):
            n = min(256, widths[i] - k)
            got = nn(left, wide[:, offsets[i] + k : offsets[i] + k + n])
            got = got[:SLOT] + got[SLOT:]
            for j in range(n // LANES):
                grads[pl.ds(firsts[i] + k // LANES + j, ranks, stride=block), :] = got[
                    :ranks, j * LANES : (j + 1) * LANES
                ]

    wide_block = NY * block
    copies = []
    for k in list(range(1, NZL)) + [0]:
        z_ = (zl + k) % NZL
        at = pl.multiple_of(((1 - c) * NZL + z_) * wide_block, 8)
        copy = remote(
            grads.at[pl.ds(at, wide_block)],
            pair_in.at[z_],
            pair_send.at[k],
            pair_recv.at[k],
            dp=dp_of(zl, y, 1 - c),
        )
        copy.start()
        copies.append(copy)
    sends += copies
    y_copies = {}
    for copy, k in zip(copies, list(range(1, NZL)) + [0]):
        z_ = (zl + k) % NZL
        at = pl.multiple_of((c * NZL + z_) * wide_block, 8)
        copy.wait_recv()
        pair_sum[z_] = (grads[pl.ds(at, wide_block), :] + pair_in[z_]).reshape(NY, block, LANES)
        for j in range(1, NY):
            y_ = (y + j) % NY
            copy = remote(
                pair_sum.at[z_, y_],
                y_in.at[z_, y],
                y_send.at[k, j],
                y_recv.at[k, j],
                dp=dp_of(zl, y_, c),
            )
            copy.start()
            y_copies[k, j] = copy
    z_copies = []
    for k in list(range(1, NZL)) + [0]:
        z_ = (zl + k) % NZL
        held = pair_sum[z_, y]
        for j in range(1, NY):
            y_copies[k, j].wait_recv()
            sends.append(y_copies[k, j])
        for j in range(1, NY):
            held += y_in[z_, (y + j) % NY]
        if k:
            z_out[k] = held
            copy = remote(
                z_out.at[k], z_in.at[zl], z_send.at[k], z_recv.at[k], dp=dp_of(z_, y, c)
            )
            copy.start()
            z_copies.append(copy)
    for copy in z_copies:
        copy.wait_recv()
    for k in range(1, NZL):
        held += z_in[(zl + k) % NZL]
    out_ref[...] = held
    for copy in sends + z_copies:
        copy.wait_send()


def per_device(
    nx,
    block_input_rows,
    up_loss_gradient,
    down_projection_input,
    output_loss_gradient,
    model_side_factors,
    hidden_side_factors,
    example_index_rows,
    clipping_threshold,
    model_side_noise,
    hidden_side_noise,
):
    ndp, nblk = lax.axis_size("dp"), lax.axis_size("blk")
    NZL, NY, NC = DP_AXES[ndp]
    NX, NZH = BLK_AXES[nblk]
    tokens = block_input_rows.shape[0]
    model, hidden = block_input_rows.shape[1], up_loss_gradient.shape[1]
    widths = (model, hidden, hidden, model)
    total = sum(widths)
    rows = total // LANES
    block = -(-rows // 8) * 8
    sent = -(-rows // 16) * 16
    own = jnp.concatenate(
        [
            model_side_factors.reshape(-1, LANES),
            hidden_side_factors.reshape(-1, LANES),
            jnp.zeros((sent - rows, LANES), BF16),
        ]
    )
    cfg = (NZL, NY, NC, NX, NZH, widths, block)
    half, reach = tokens // 2, 256
    dma = pltpu.SemaphoreType.DMA
    vmem = pl.BlockSpec(memory_space=pltpu.VMEM)
    hbm = pl.BlockSpec(memory_space=pl.ANY)
    summed = pl.pallas_call(
        functools.partial(kernel, cfg),
        out_shape=jax.ShapeDtypeStruct((block, LANES), F32),
        in_specs=[pl.BlockSpec(memory_space=pltpu.SMEM), vmem, vmem, hbm, hbm, hbm, hbm],
        out_specs=vmem,
        scratch_shapes=[
            pltpu.VMEM((tokens, total), BF16),
            pltpu.VMEM((ndp, sent, LANES), BF16),
            pltpu.VMEM((ndp * block, LANES), F32),
            pltpu.VMEM((LANES, total), BF16),
            pltpu.VMEM((4, 2, half, reach), BF16),
            pltpu.VMEM((4, 2, half, reach), BF16),
            pltpu.VMEM((NX, tokens // NX, LANES), F32),
            pltpu.VMEM((NX, tokens // NX, LANES), F32),
            pltpu.VMEM((tokens // NX, LANES), F32),
            pltpu.VMEM((NZH, tokens // NX, LANES), F32),
            pltpu.VMEM((NX, tokens // NX, LANES), F32),
            pltpu.VMEM((NX * NY * NC, 1, LANES), F32),
            pltpu.VMEM((NZL * NZH, 2, LANES), F32),
            pltpu.VMEM((ndp * block, LANES), F32),
            pltpu.VMEM((NZL, NY * block, LANES), F32),
            pltpu.VMEM((NZL, NY, block, LANES), F32),
            pltpu.VMEM((NZL, NY, block, LANES), F32),
            pltpu.VMEM((NZL, block, LANES), F32),
            pltpu.VMEM((NZL, block, LANES), F32),
            dma((4,)),
            dma((ndp,)),
            dma((ndp,)),
            dma((NX,)),
            dma((NX,)),
            dma((NZH,)),
            dma((NZH,)),
            dma((NX,)),
            dma((NX,)),
            dma,
            dma,
            dma,
            dma,
            dma((NZL,)),
            dma((NZL,)),
            dma((NZL, NY)),
            dma((NZL, NY)),
            dma((NZL,)),
            dma((NZL,)),
        ],
        compiler_params=pltpu.CompilerParams(
            collective_id=0, has_side_effects=True, vmem_limit_bytes=56 << 20
        ),
        name="clipped_step",
    )(
        clipping_threshold,
        example_index_rows,
        own,
        block_input_rows,
        up_loss_gradient,
        down_projection_input,
        output_loss_gradient,
    )
    cut = 2 * model // LANES
    return (
        summed[:cut].reshape(model_side_noise.shape) + model_side_noise,
        summed[cut:rows].reshape(hidden_side_noise.shape) + hidden_side_noise,
    )


def solution(mesh):
    in_specs = (
        P("dp", "blk"),
        P("dp", "blk"),
        P("dp", "blk"),
        P("dp", "blk"),
        P(None, "dp", "blk"),
        P(None, "dp", "blk"),
        P("dp", None),
        P(),
        P(None, "dp", "blk"),
        P(None, "dp", "blk"),
    )
    out_specs = (P(None, "dp", "blk"), P(None, "dp", "blk"))
    return jax.shard_map(
        functools.partial(per_device, None),
        mesh=mesh,
        in_specs=in_specs,
        out_specs=out_specs,
        check_vma=False,
    )
```

```python
import functools
import math

import jax
import jax.numpy as jnp
from jax import lax
from jax.experimental import pallas as pl
from jax.experimental.pallas import tpu as pltpu
from jax.sharding import PartitionSpec as P

EX = 8
LANES = 128
SLOT = 32
DP_AXES = {32: (4, 4, 2), 4: (2, 1, 2), 8: (2, 2, 2), 16: (2, 4, 2)}
BLK_AXES = {16: (4, 4), 4: (2, 2), 2: (1, 2), 1: (1, 1)}
PAIR = (1, 0, 3, 2)
BAND = 48
F32 = jnp.float32
BF16 = jnp.bfloat16


def nt(a, b):
    return lax.dot_general(a, b, (((1,), (1,)), ((), ())), preferred_element_type=F32)


def nn(a, b):
    return lax.dot_general(a, b, (((1,), (0,)), ((), ())), preferred_element_type=F32)


def split(a):
    high = a.astype(BF16)
    return high, (a - high.astype(F32)).astype(BF16)


def remote(src, dst, send, recv, **where):
    return pltpu.make_async_remote_copy(
        src_ref=src,
        dst_ref=dst,
        send_sem=send,
        recv_sem=recv,
        device_id=where,
        device_id_type=pl.DeviceIdType.MESH,
    )


def kernel(
    cfg,
    thr_ref,
    ids_ref,
    model_ref,
    hidden_ref,
    a0,
    a1,
    a2,
    a3,
    model_out,
    hidden_out,
    wide,
    row_f32,
    row_ref,
    rows_in,
    rows_f32,
    factors,
    gram,
    gram_in,
    gram_hi,
    gram_lo,
    part,
    part_in,
    quarter,
    quarter_in,
    proj,
    plane,
    ring,
    left,
    singles,
    grads,
    pair_in,
    pair_sum,
    y_in,
    z_out,
    z_in,
    load_sem,
    row_send,
    row_recv,
    gram_send,
    gram_recv,
    part_send,
    part_recv,
    quarter_send,
    quarter_recv,
    proj_send,
    proj_recv,
    plane_send,
    plane_recv,
    ring_send,
    ring_recv,
    pair_send,
    pair_recv,
    y_send,
    y_recv,
    z_send,
    z_recv,
    token,
):
    NZL, NY, NC, NX, NZH, widths, block = cfg
    tokens = wide.shape[0]
    ranks = NZL * NY * NC
    dp, blk = lax.axis_index("dp"), lax.axis_index("blk")
    zl, y, c = dp // (NY * NC), (dp // NC) % NY, dp % NC
    x, zh = blk // NZH, blk % NZH
    nz, npl = NZL * NZH, NX * NY * NC
    zz = zh * NZL + zl
    pp = (x * NY + y) * NC + c
    zls = [lax.rem(zl + k, NZL) for k in range(NZL)]
    zhs = [lax.rem(zh + k, NZH) for k in range(NZH)]
    xs = [lax.rem(x + k, NX) for k in range(NX)]
    ys = [lax.rem(y + k, NY) for k in range(NY)]
    cs = [c, 1 - c]

    def dp_of(z_, y_, c_):
        return (z_ * NY + y_) * NC + c_

    def slot_of(z_, y_, c_):
        return (c_ * NZL + z_) * NY + y_

    def signal(semaphore, **where):
        pl.semaphore_signal(
            semaphore, inc=1, device_id=where, device_id_type=pl.DeviceIdType.MESH
        )

    def signal_along(semaphore, distance):
        for k in (distance % nz, -distance % nz):
            q = lax.rem(zz + k, nz)
            q_hi = q // NZL
            signal(semaphore, dp=dp_of(q - q_hi * NZL, y, c), blk=x * NZH + q_hi)

    offsets = [sum(widths[:i]) for i in range(4)]
    loads = []
    for i, ref in enumerate((a0, a1, a2, a3)):
        copy = pltpu.make_async_copy(
            ref, wide.at[:, pl.ds(offsets[i], widths[i])], load_sem.at[i]
        )
        copy.start()
        loads.append(copy)

    barrier = pltpu.get_barrier_semaphore()

    for k in range(1, NZL):
        signal(barrier, dp=dp_of(zls[k], y, c))
    for k in range(1, NY):
        signal(barrier, dp=dp_of(zl, ys[k], c))
    for k in range(1, NX):
        signal(barrier, blk=xs[k] * NZH + zh)
    signal(barrier, dp=dp_of(zl, y, 1 - c))
    signal_along(barrier, 2)

    row_f32[...] = jnp.zeros_like(row_f32)
    at = 0
    for ref in (model_ref, hidden_ref):
        for k in range(2):
            for j in range(ref.shape[1] // LANES):
                row_f32[at : at + 1, :] = ref[k : k + 1, j * LANES : (j + 1) * LANES].astype(F32)
                at += 1
    row_ref[...] = row_f32[...].astype(BF16)

    half, reach = tokens // 2, 256
    member_t = (
        jnp.broadcast_to(ids_ref[...], (LANES, tokens))
        == lax.broadcasted_iota(jnp.int32, (LANES, tokens), 0)
    ).astype(F32).astype(BF16)
    eye = (
        lax.broadcasted_iota(jnp.int32, (tokens, tokens), 0)
        == lax.broadcasted_iota(jnp.int32, (tokens, tokens), 1)
    ).astype(F32).astype(BF16)
    member = nt(eye, member_t)
    member_b = member.astype(BF16)
    starts = (0, tokens - reach)
    factors[...] = jnp.zeros_like(factors)

    count = 4 // NX
    tiles = tokens // BAND
    band = [min(b * BAND, tokens - LANES) for b in range(tiles)]
    for i in (0, 3, 1, 2):
        loads[i].wait()
        for b in range(2):
            total = jnp.zeros((half, reach), F32)
            for k in range(0, widths[i], 256):
                n = min(256, widths[i] - k)
                at = offsets[i] + k
                total += nt(
                    wide[b * half : (b + 1) * half, at : at + n],
                    wide[starts[b] : starts[b] + reach, at : at + n],
                )
            for tile in range(b * tiles // 2, (b + 1) * tiles // 2):
                down = tile * BAND - b * half
                right = band[tile] - starts[b]
                gram[PAIR[i] // count, PAIR[i] % count, tile] = total[
                    down : down + BAND, right : right + LANES
                ]

    pl.semaphore_wait(barrier, NZL + NY + NX)
    signal_along(token.at[0], 2)

    own = slot_of(zl, y, c)
    sends = []

    def row_copy(src, slot, where):
        copy = remote(src, rows_in.at[slot], row_send.at[len(sends)], row_recv.at[slot], dp=where)
        copy.start()
        sends.append(copy)

    def row_wait(slot):
        remote(
            rows_in.at[slot], rows_in.at[slot], row_send.at[0], row_recv.at[slot], dp=dp_of(zl, y, 1 - c)
        ).wait_recv()

    for k in range(1, NZL):
        row_copy(row_ref, own, dp_of(zls[k], y, c))
    for j in range(1, NY):
        row_copy(row_ref, own, dp_of(zl, ys[j], c))
    row_copy(row_ref, own, dp_of(zl, y, 1 - c))
    gram_copies = []
    for k in range(1, NX):
        copy = remote(
            gram.at[xs[k]], gram_in.at[x], gram_send.at[k], gram_recv.at[k], blk=xs[k] * NZH + zh
        )
        copy.start()
        gram_copies.append(copy)

    for k in range(1, NZL):
        z_ = zls[k]
        slot = slot_of(z_, y, c)
        row_wait(slot)
        for j in range(1, NY):
            row_copy(rows_in.at[slot], slot, dp_of(zl, ys[j], c))
        row_copy(rows_in.at[slot], slot, dp_of(zl, y, 1 - c))
    for k in range(NZL):
        for j in range(1, NY):
            slot = slot_of(zls[k], ys[j], c)
            row_wait(slot)
            row_copy(rows_in.at[slot], slot, dp_of(zl, y, 1 - c))

    pl.semaphore_wait(token.at[0], 2)
    signal_along(token.at[1], 4)

    def widen(ref, slot):
        at = pl.multiple_of(slot * block, 8)
        rows_f32[pl.ds(at, block), :] = ref[...].astype(F32)[:block]

    widen(row_ref, own)
    for k in range(NZL):
        for j in range(NY):
            if k or j:
                slot = slot_of(zls[k], ys[j], c)
                widen(rows_in.at[slot], slot)
    for k in range(NZL):
        for j in range(NY):
            slot = slot_of(zls[k], ys[j], 1 - c)
            row_wait(slot)
            widen(rows_in.at[slot], slot)

    chunks = [w // LANES for w in widths]
    firsts = (0, chunks[0] + chunks[3], chunks[0] + chunks[3] + chunks[1], chunks[0])
    for i in range(4):
        for j in range(chunks[i]):
            picked = rows_f32[pl.ds(firsts[i] + j, ranks, stride=block), :]
            at = offsets[i] + j * LANES
            factors[SLOT * i : SLOT * i + ranks, at : at + LANES] = picked.astype(BF16)

    total = jnp.zeros((tokens, LANES), F32)
    for k in range(0, wide.shape[1], 256):
        n = min(256, wide.shape[1] - k)
        total += nt(wide[:, k : k + n], factors[:, k : k + n])
    lane = lax.broadcasted_iota(jnp.int32, (tokens // 4, LANES), 1) // SLOT
    for q in range(4):
        packed = jnp.zeros((tokens // 4, LANES), F32)
        for g in range(4):
            piece = total[g * tokens // 4 : (g + 1) * tokens // 4]
            if g != q:
                piece = pltpu.roll(piece, SLOT * (g - q) % LANES, 1)
            packed = jnp.where(lane == g, piece, packed)
        part[q // count, q % count] = packed

    copies = []
    for k in range(1, NX):
        x_ = xs[k]
        copy = remote(
            part.at[x_], part_in.at[x], part_send.at[k], part_recv.at[k], blk=x_ * NZH + zh
        )
        copy.start()
        copies.append(copy)
    for copy in gram_copies:
        copy.wait_recv()
    sends += gram_copies
    for tile in range(tiles):
        own_at = tile * BAND
        same = nt(member_b[own_at : own_at + BAND], member_b[band[tile] : band[tile] + LANES])
        ahead = (
            band[tile]
            - own_at
            + lax.broadcasted_iota(jnp.int32, (BAND, LANES), 1)
            - lax.broadcasted_iota(jnp.int32, (BAND, LANES), 0)
        )
        times = jnp.where(ahead > 0, 2.0, jnp.where(ahead == 0, 1.0, 0.0)) * same
        for q in range(count):
            total = gram[x, q, tile]
            for k in range(1, NX):
                total += gram_in[xs[k], q, tile]
            high, low = split(times * total)
            gram_hi[q, tile] = high
            gram_lo[q, tile] = low
    for copy in copies:
        copy.wait_recv()
    pl.semaphore_wait(token.at[1], 2)
    held = part[x]
    for k in range(1, NX):
        held += part_in[xs[k]]
    quarter[...] = held
    sends += copies
    copies = []
    for k in range(1, NZH):
        copy = remote(
            quarter,
            quarter_in.at[zh],
            quarter_send.at[k],
            quarter_recv.at[k],
            blk=x * NZH + zhs[k],
        )
        copy.start()
        copies.append(copy)
    for copy in copies:
        copy.wait_recv()
    for k in range(1, NZH):
        held += quarter_in[zhs[k]]
    proj[x] = held
    sends += copies
    copies = []
    for k in range(1, NX):
        copy = remote(
            proj.at[x], proj.at[x], proj_send.at[k], proj_recv.at[k], blk=(xs[k]) * NZH + zh
        )
        copy.start()
        copies.append(copy)

    norm = jnp.zeros((1, LANES), F32)
    for q in range(count):
        mine = jnp.concatenate(
            [
                jnp.where(lane == 0, held[q] if g == 0 else pltpu.roll(held[q], LANES - SLOT * g, 1), 0.0)
                for g in range(4)
            ],
            axis=0,
        )
        high = mine.astype(BF16).astype(F32)
        both = (high + pltpu.roll(mine - high, SLOT, 1)).astype(BF16)
        for tile in range(tiles):
            near = both[band[tile] : band[tile] + LANES]
            mixed = nn(gram_hi[q, tile], near) + nn(gram_lo[q, tile], near)
            mixed += pltpu.roll(mixed, LANES - SLOT, 1)
            own_at = tile * BAND
            each = jnp.sum(mixed * mine[own_at : own_at + BAND], axis=1, keepdims=True)
            norm += jnp.sum(member[own_at : own_at + BAND] * each, axis=0, keepdims=True)

    plane[pp] = norm

    for k in range(NX):
        for j in range(NY):
            for i in range(NC):
                if k or j or i:
                    remote(
                        plane.at[pp],
                        plane.at[pp],
                        plane_send,
                        plane_recv,
                        dp=dp_of(zl, ys[j], cs[i]),
                        blk=xs[k] * NZH + zh,
                    ).start()

    for copy in copies:
        copy.wait_recv()
    sends += copies
    pieces = []
    for g in range(4):
        piece = jnp.zeros((tokens // 4, LANES), F32)
        for q in range(4):
            packed = proj[q // count, q % count]
            if g != q:
                packed = pltpu.roll(packed, SLOT * (q - g) % LANES, 1)
            piece = jnp.where(lane == q, packed, piece)
        pieces.append(piece)
    high, low = split(jnp.concatenate(pieces, axis=0))
    eye = (
        lax.broadcasted_iota(jnp.int32, (LANES, LANES), 0)
        == lax.broadcasted_iota(jnp.int32, (LANES, LANES), 1)
    ).astype(F32).astype(BF16)
    high_t, low_t = nt(eye, high), nt(eye, low)
    for e in range(EX):
        here = jnp.broadcast_to(ids_ref[...], (SLOT, tokens)) == e
        for i in range(4):
            at = SLOT * PAIR[i]
            for n, part_t in enumerate((high_t, low_t)):
                left[i, (2 * e + n) * SLOT : (2 * e + n + 1) * SLOT] = jnp.where(
                    here, part_t[at : at + SLOT], 0.0
                ).astype(BF16)

    rest = plane.at[pl.ds(0, npl - 1)]
    remote(rest, rest, plane_send, plane_recv, dp=dp_of(zl, y, 1 - c)).wait()
    everyone = jnp.sum(plane[...], axis=0)
    group = jnp.zeros((1, LANES), F32)
    for k in range(NX):
        group += plane[(k * NY + y) * NC + c]
    ring[zz] = jnp.concatenate([group, everyone], axis=0)

    for k in sorted(range(NZH), key=lambda d: -min(d, NZH - d)):
        for j in range(NZL):
            if k or j:
                remote(
                    ring.at[zz],
                    ring.at[zz],
                    ring_send,
                    ring_recv,
                    dp=dp_of(zls[j], y, c),
                    blk=x * NZH + zhs[k],
                ).start()

    for i in range(4):
        step = 256 if widths[i] % 256 == 0 else LANES
        for k in range(0, widths[i], step):
            at = offsets[i] + k
            got = nn(left[i], wide[:, at : at + step]).reshape(EX, 2, SLOT // 8, 8, step)
            singles[:, :, :, at : at + step] = got[:, 0] + got[:, 1]

    rest = ring.at[pl.ds(0, nz - 1)]
    remote(rest, rest, ring_send, ring_recv, dp=dp_of(zl, y, 1 - c)).wait()
    everyone = jnp.sum(ring[...], axis=0)[1:2]
    group = jnp.zeros((1, LANES), F32)
    for k in range(NZH):
        group += ring[k * NZL + zl][0:1]
    grand_total = jnp.sum(everyone, axis=1, keepdims=True)
    root_mean = jnp.sqrt(jnp.maximum(grand_total, 0.0) / (ranks * EX) + 1e-06)
    clip = (0.5 + 0.125 * thr_ref[...].astype(F32)) * root_mean
    factor = jnp.minimum(1.0, clip * lax.rsqrt(jnp.maximum(group, 0.0) + 1e-06))
    entries = 2 * ranks * NX * NZH * (widths[0] + widths[1])
    rescale = math.sqrt(entries / (ranks * EX)) / clip
    scaled = factor * rescale
    lane = lax.broadcasted_iota(jnp.int32, (1, LANES), 1)
    weights = [
        jnp.broadcast_to(
            jnp.sum(jnp.where(lane == e, scaled, 0.0), axis=1, keepdims=True), (8, LANES)
        )
        for e in range(EX)
    ]

    def clipped(g):
        for i in range(4):
            for j in range(chunks[i]):
                at = offsets[i] + j * LANES
                total = weights[0] * singles[0, g, :, at : at + LANES]
                for e in range(1, EX):
                    total += weights[e] * singles[e, g, :, at : at + LANES]
                grads[pl.ds(g * (8 * block) + firsts[i] + j, 8, stride=block), :] = total

    wide_block = NY * block
    groups = NZL * NY // 8
    if groups == 2:
        pair_at = zl // 2
        away = 2 * lax.rem(pair_at + 1, 2)
        other = 2 * pair_at + 1 - lax.rem(zl, 2)
        order = [away, away + 1, other, zl]
        sets = [lax.rem(pair_at + 1, 2), pair_at]
    else:
        order = [1 - zl, zl]
        sets = [0] * groups
        if not groups:
            for g in range(-(-ranks // 8)):
                clipped(g)
    batch = len(order) // max(groups, 1)
    copies = []
    for n in range(max(groups, 1)):
        if groups:
            clipped((1 - c) * groups + sets[n])
        for o in range(n * batch, (n + 1) * batch):
            at = pl.multiple_of(((1 - c) * NZL + order[o]) * wide_block, 8)
            copy = remote(
                grads.at[pl.ds(at, wide_block)],
                pair_in.at[o],
                pair_send.at[o],
                pair_recv.at[o],
                dp=dp_of(zl, y, 1 - c),
            )
            copy.start()
            copies.append(copy)
    sends += copies
    y_copies = {}
    for n in range(max(groups, 1)):
        if groups:
            clipped(c * groups + sets[n])
        for o in range(n * batch, (n + 1) * batch):
            at = pl.multiple_of((c * NZL + order[o]) * wide_block, 8)
            copies[o].wait_recv()
            pair_sum[o] = (grads[pl.ds(at, wide_block), :] + pair_in[o]).reshape(NY, block, LANES)
            for j in range(1, NY):
                copy = remote(
                    pair_sum.at[o, ys[j]],
                    y_in.at[o, y],
                    y_send.at[o, j],
                    y_recv.at[o, j],
                    dp=dp_of(zl, ys[j], c),
                )
                copy.start()
                y_copies[o, j] = copy
    last = NZL - 1
    for o in range(NZL):
        held = pair_sum[o, y]
        for j in range(1, NY):
            y_copies[o, j].wait_recv()
            sends.append(y_copies[o, j])
        for j in range(1, NY):
            held += y_in[o, ys[j]]
        if o < last:
            z_out[o] = held
            copy = remote(
                z_out.at[o], z_in.at[zl], z_send.at[o], z_recv.at[zl], dp=dp_of(order[o], y, c)
            )
            copy.start()
            sends.append(copy)
    for k in range(1, NZL):
        remote(
            z_in.at[zls[k]], z_in.at[zls[k]], z_send.at[0], z_recv.at[zls[k]], dp=dp_of(zl, y, 1 - c)
        ).wait_recv()
    for k in range(1, NZL):
        held += z_in[zls[k]]
    row_f32[: held.shape[0], :] = held
    at = 0
    for ref in (model_out, hidden_out):
        for k in range(2):
            for j in range(ref.shape[2] // LANES):
                ref[k, :, j * LANES : (j + 1) * LANES] = row_f32[at : at + 1, :]
                at += 1
    for copy in sends:
        copy.wait_send()


def per_device(
    block_input_rows,
    up_loss_gradient,
    down_projection_input,
    output_loss_gradient,
    model_side_factors,
    hidden_side_factors,
    example_index_rows,
    clipping_threshold,
    model_side_noise,
    hidden_side_noise,
):
    ndp, nblk = lax.axis_size("dp"), lax.axis_size("blk")
    NZL, NY, NC = DP_AXES[ndp]
    NX, NZH = BLK_AXES[nblk]
    tokens = block_input_rows.shape[0]
    model, hidden = block_input_rows.shape[1], up_loss_gradient.shape[1]
    widths = (model, hidden, hidden, model)
    total = sum(widths)
    rows = total // LANES
    block = -(-rows // 8) * 8
    sent = -(-rows // 16) * 16
    cfg = (NZL, NY, NC, NX, NZH, widths, block)
    count, tiles = 4 // NX, tokens // BAND
    dma = pltpu.SemaphoreType.DMA
    vmem = pl.BlockSpec(memory_space=pltpu.VMEM)
    hbm = pl.BlockSpec(memory_space=pl.ANY)
    summed = pl.pallas_call(
        functools.partial(kernel, cfg),
        out_shape=[
            jax.ShapeDtypeStruct(model_side_noise.shape, F32),
            jax.ShapeDtypeStruct(hidden_side_noise.shape, F32),
        ],
        in_specs=[vmem, vmem, vmem, vmem, hbm, hbm, hbm, hbm],
        out_specs=[vmem, vmem],
        scratch_shapes=[
            pltpu.VMEM((tokens, total), BF16),
            pltpu.VMEM((sent, LANES), F32),
            pltpu.VMEM((sent, LANES), BF16),
            pltpu.VMEM((ndp, sent, LANES), BF16),
            pltpu.VMEM((ndp * block, LANES), F32),
            pltpu.VMEM((LANES, total), BF16),
            pltpu.VMEM((NX, count, tiles, BAND, LANES), F32),
            pltpu.VMEM((NX, count, tiles, BAND, LANES), F32),
            pltpu.VMEM((count, tiles, BAND, LANES), BF16),
            pltpu.VMEM((count, tiles, BAND, LANES), BF16),
            pltpu.VMEM((NX, count, tokens // 4, LANES), F32),
            pltpu.VMEM((NX, count, tokens // 4, LANES), F32),
            pltpu.VMEM((count, tokens // 4, LANES), F32),
            pltpu.VMEM((NZH, count, tokens // 4, LANES), F32),
            pltpu.VMEM((NX, count, tokens // 4, LANES), F32),
            pltpu.VMEM((NX * NY * NC, 1, LANES), F32),
            pltpu.VMEM((NZL * NZH, 2, LANES), F32),
            pltpu.VMEM((4, 2 * EX * SLOT, tokens), BF16),
            pltpu.VMEM((EX, SLOT // 8, 8, total), F32),
            pltpu.VMEM((ndp * block, LANES), F32),
            pltpu.VMEM((NZL, NY * block, LANES), F32),
            pltpu.VMEM((NZL, NY, block, LANES), F32),
            pltpu.VMEM((NZL, NY, block, LANES), F32),
            pltpu.VMEM((NZL, block, LANES), F32),
            pltpu.VMEM((NZL, block, LANES), F32),
            dma((4,)),
            dma((ndp,)),
            dma((ndp,)),
            dma((NX,)),
            dma((NX,)),
            dma((NX,)),
            dma((NX,)),
            dma((NZH,)),
            dma((NZH,)),
            dma((NX,)),
            dma((NX,)),
            dma,
            dma,
            dma,
            dma,
            dma((NZL,)),
            dma((NZL,)),
            dma((NZL, NY)),
            dma((NZL, NY)),
            dma((NZL,)),
            dma((NZL,)),
            pltpu.SemaphoreType.REGULAR((2,)),
        ],
        compiler_params=pltpu.CompilerParams(
            collective_id=0, has_side_effects=True, vmem_limit_bytes=56 << 20
        ),
        name="clipped_step",
    )(
        clipping_threshold.reshape(1, 1),
        example_index_rows,
        model_side_factors.reshape(2, model),
        hidden_side_factors.reshape(2, hidden),
        block_input_rows,
        up_loss_gradient,
        down_projection_input,
        output_loss_gradient,
    )
    return (summed[0] + model_side_noise, summed[1] + hidden_side_noise)


def solution(mesh):
    in_specs = (
        P("dp", "blk"),
        P("dp", "blk"),
        P("dp", "blk"),
        P("dp", "blk"),
        P(None, "dp", "blk"),
        P(None, "dp", "blk"),
        P("dp", None),
        P(),
        P(None, "dp", "blk"),
        P(None, "dp", "blk"),
    )
    out_specs = (P(None, "dp", "blk"), P(None, "dp", "blk"))
    return jax.shard_map(
        per_device,
        mesh=mesh,
        in_specs=in_specs,
        out_specs=out_specs,
        check_vma=False,
    )
```

```python
import functools
import math

import jax
import jax.numpy as jnp
from jax import lax
from jax.experimental import pallas as pl
from jax.experimental.pallas import tpu as pltpu
from jax.sharding import PartitionSpec as P

EX = 8
LANES = 128
SLOT = 32
DP_AXES = {32: (4, 4, 2), 4: (2, 1, 2), 8: (2, 2, 2), 16: (2, 4, 2)}
BLK_AXES = {16: (4, 4), 4: (2, 2), 2: (1, 2), 1: (1, 1)}
PAIR = (1, 0, 3, 2)
BAND = 48
F32 = jnp.float32
BF16 = jnp.bfloat16


def nt(a, b):
    return lax.dot_general(a, b, (((1,), (1,)), ((), ())), preferred_element_type=F32)


def nn(a, b):
    return lax.dot_general(a, b, (((1,), (0,)), ((), ())), preferred_element_type=F32)


def split(a):
    high = a.astype(BF16)
    return high, (a - high.astype(F32)).astype(BF16)


def remote(src, dst, send, recv, **where):
    return pltpu.make_async_remote_copy(
        src_ref=src,
        dst_ref=dst,
        send_sem=send,
        recv_sem=recv,
        device_id=where,
        device_id_type=pl.DeviceIdType.MESH,
    )


def kernel(
    cfg,
    thr_ref,
    ids_ref,
    model_ref,
    hidden_ref,
    a0,
    a1,
    a2,
    a3,
    model_out,
    hidden_out,
    wide,
    row_f32,
    row_ref,
    rows_in,
    rows_f32,
    factors,
    gram,
    gram_in,
    gram_hi,
    gram_lo,
    part,
    part_in,
    quarter,
    quarter_in,
    proj,
    plane,
    ring,
    left,
    singles,
    grads,
    pair_in,
    pair_sum,
    y_in,
    z_out,
    z_in,
    load_sem,
    row_send,
    row_recv,
    gram_send,
    gram_recv,
    part_send,
    part_recv,
    quarter_send,
    quarter_recv,
    proj_send,
    proj_recv,
    plane_send,
    plane_recv,
    ring_send,
    ring_recv,
    pair_send,
    pair_recv,
    y_send,
    y_recv,
    z_send,
    z_recv,
    token,
):
    NZL, NY, NC, NX, NZH, widths, block = cfg
    tokens = wide.shape[0]
    ranks = NZL * NY * NC
    dp, blk = lax.axis_index("dp"), lax.axis_index("blk")
    zl, y, c = dp // (NY * NC), (dp // NC) % NY, dp % NC
    x, zh = blk // NZH, blk % NZH
    nz, npl = NZL * NZH, NX * NY * NC
    zz = zh * NZL + zl
    pp = (x * NY + y) * NC + c
    zls = [lax.rem(zl + k, NZL) for k in range(NZL)]
    zhs = [lax.rem(zh + k, NZH) for k in range(NZH)]
    xs = [lax.rem(x + k, NX) for k in range(NX)]
    ys = [lax.rem(y + k, NY) for k in range(NY)]
    cs = [c, 1 - c]

    def dp_of(z_, y_, c_):
        return (z_ * NY + y_) * NC + c_

    def slot_of(z_, y_, c_):
        return (c_ * NZL + z_) * NY + y_

    def signal(semaphore, **where):
        pl.semaphore_signal(
            semaphore, inc=1, device_id=where, device_id_type=pl.DeviceIdType.MESH
        )

    def signal_along(semaphore, distance):
        for k in (distance % nz, -distance % nz):
            q = lax.rem(zz + k, nz)
            q_hi = q // NZL
            signal(semaphore, dp=dp_of(q - q_hi * NZL, y, c), blk=x * NZH + q_hi)

    offsets = [sum(widths[:i]) for i in range(4)]
    loads = []
    for i, ref in enumerate((a0, a1, a2, a3)):
        copy = pltpu.make_async_copy(
            ref, wide.at[:, pl.ds(offsets[i], widths[i])], load_sem.at[i]
        )
        copy.start()
        loads.append(copy)

    barrier = pltpu.get_barrier_semaphore()

    for k in range(1, NZL):
        signal(barrier, dp=dp_of(zls[k], y, c))
    for k in range(1, NY):
        signal(barrier, dp=dp_of(zl, ys[k], c))
    for k in range(1, NX):
        signal(barrier, blk=xs[k] * NZH + zh)
    signal(barrier, dp=dp_of(zl, y, 1 - c))
    signal_along(barrier, 2)

    row_f32[...] = jnp.zeros_like(row_f32)
    at = 0
    for ref in (model_ref, hidden_ref):
        for k in range(2):
            for j in range(ref.shape[1] // LANES):
                row_f32[at : at + 1, :] = ref[k : k + 1, j * LANES : (j + 1) * LANES].astype(F32)
                at += 1
    row_ref[...] = row_f32[...].astype(BF16)

    half, reach = tokens // 2, 256
    member_t = (
        jnp.broadcast_to(ids_ref[...], (LANES, tokens))
        == lax.broadcasted_iota(jnp.int32, (LANES, tokens), 0)
    ).astype(F32).astype(BF16)
    eye = (
        lax.broadcasted_iota(jnp.int32, (tokens, tokens), 0)
        == lax.broadcasted_iota(jnp.int32, (tokens, tokens), 1)
    ).astype(F32).astype(BF16)
    member = nt(eye, member_t)
    member_b = member.astype(BF16)
    starts = (0, tokens - reach)
    factors[...] = jnp.zeros_like(factors)

    count = 4 // NX
    tiles = tokens // BAND
    band = [min(b * BAND, tokens - LANES) for b in range(tiles)]
    for i in (0, 3, 1, 2):
        loads[i].wait()
        for b in range(2):
            total = jnp.zeros((half, reach), F32)
            for k in range(0, widths[i], 256):
                n = min(256, widths[i] - k)
                at = offsets[i] + k
                total += nt(
                    wide[b * half : (b + 1) * half, at : at + n],
                    wide[starts[b] : starts[b] + reach, at : at + n],
                )
            for tile in range(b * tiles // 2, (b + 1) * tiles // 2):
                down = tile * BAND - b * half
                right = band[tile] - starts[b]
                gram[PAIR[i] // count, PAIR[i] % count, tile] = total[
                    down : down + BAND, right : right + LANES
                ]

    pl.semaphore_wait(barrier, NZL + NY + NX)
    signal_along(token.at[0], 2)

    own = slot_of(zl, y, c)
    sends = []

    def row_copy(src, slot, where):
        copy = remote(src, rows_in.at[slot], row_send.at[len(sends)], row_recv.at[slot], dp=where)
        copy.start()
        sends.append(copy)

    def row_wait(slot):
        remote(
            rows_in.at[slot], rows_in.at[slot], row_send.at[0], row_recv.at[slot], dp=dp_of(zl, y, 1 - c)
        ).wait_recv()

    for k in range(1, NZL):
        row_copy(row_ref, own, dp_of(zls[k], y, c))
    for j in range(1, NY):
        row_copy(row_ref, own, dp_of(zl, ys[j], c))
    row_copy(row_ref, own, dp_of(zl, y, 1 - c))
    gram_copies = []
    for k in range(1, NX):
        copy = remote(
            gram.at[xs[k]], gram_in.at[x], gram_send.at[k], gram_recv.at[k], blk=xs[k] * NZH + zh
        )
        copy.start()
        gram_copies.append(copy)

    for k in range(1, NZL):
        z_ = zls[k]
        slot = slot_of(z_, y, c)
        row_wait(slot)
        for j in range(1, NY):
            row_copy(rows_in.at[slot], slot, dp_of(zl, ys[j], c))
        row_copy(rows_in.at[slot], slot, dp_of(zl, y, 1 - c))
    for k in range(NZL):
        for j in range(1, NY):
            slot = slot_of(zls[k], ys[j], c)
            row_wait(slot)
            row_copy(rows_in.at[slot], slot, dp_of(zl, y, 1 - c))

    pl.semaphore_wait(token.at[0], 2)
    signal_along(token.at[1], 4)

    def widen(ref, slot):
        at = pl.multiple_of(slot * block, 8)
        rows_f32[pl.ds(at, block), :] = ref[...].astype(F32)[:block]

    widen(row_ref, own)
    for k in range(NZL):
        for j in range(NY):
            if k or j:
                slot = slot_of(zls[k], ys[j], c)
                widen(rows_in.at[slot], slot)
    for k in range(NZL):
        for j in range(NY):
            slot = slot_of(zls[k], ys[j], 1 - c)
            row_wait(slot)
            widen(rows_in.at[slot], slot)

    chunks = [w // LANES for w in widths]
    firsts = (0, chunks[0] + chunks[3], chunks[0] + chunks[3] + chunks[1], chunks[0])
    for i in range(4):
        for j in range(chunks[i]):
            picked = rows_f32[pl.ds(firsts[i] + j, ranks, stride=block), :]
            at = offsets[i] + j * LANES
            factors[SLOT * i : SLOT * i + ranks, at : at + LANES] = picked.astype(BF16)

    total = jnp.zeros((tokens, LANES), F32)
    for k in range(0, wide.shape[1], 256):
        n = min(256, wide.shape[1] - k)
        total += nt(wide[:, k : k + n], factors[:, k : k + n])
    lane = lax.broadcasted_iota(jnp.int32, (tokens // 4, LANES), 1) // SLOT
    for q in range(4):
        packed = jnp.zeros((tokens // 4, LANES), F32)
        for g in range(4):
            piece = total[g * tokens // 4 : (g + 1) * tokens // 4]
            if g != q:
                piece = pltpu.roll(piece, SLOT * (g - q) % LANES, 1)
            packed = jnp.where(lane == g, piece, packed)
        part[q // count, q % count] = packed

    copies = []
    for k in range(1, NX):
        x_ = xs[k]
        copy = remote(
            part.at[x_], part_in.at[x], part_send.at[k], part_recv.at[k], blk=x_ * NZH + zh
        )
        copy.start()
        copies.append(copy)
    for copy in gram_copies:
        copy.wait_recv()
    sends += gram_copies
    for tile in range(tiles):
        own_at = tile * BAND
        same = nt(member_b[own_at : own_at + BAND], member_b[band[tile] : band[tile] + LANES])
        ahead = (
            band[tile]
            - own_at
            + lax.broadcasted_iota(jnp.int32, (BAND, LANES), 1)
            - lax.broadcasted_iota(jnp.int32, (BAND, LANES), 0)
        )
        times = jnp.where(ahead > 0, 2.0, jnp.where(ahead == 0, 1.0, 0.0)) * same
        for q in range(count):
            total = gram[x, q, tile]
            for k in range(1, NX):
                total += gram_in[xs[k], q, tile]
            high, low = split(times * total)
            gram_hi[q, tile] = high
            gram_lo[q, tile] = low
    for copy in copies:
        copy.wait_recv()
    pl.semaphore_wait(token.at[1], 2)
    held = part[x]
    for k in range(1, NX):
        held += part_in[xs[k]]
    quarter[...] = held
    sends += copies
    copies = []
    for k in range(1, NZH):
        copy = remote(
            quarter,
            quarter_in.at[zh],
            quarter_send.at[k],
            quarter_recv.at[k],
            blk=x * NZH + zhs[k],
        )
        copy.start()
        copies.append(copy)
    for copy in copies:
        copy.wait_recv()
    for k in range(1, NZH):
        held += quarter_in[zhs[k]]
    proj[x] = held
    sends += copies
    copies = []
    for k in range(1, NX):
        copy = remote(
            proj.at[x], proj.at[x], proj_send.at[k], proj_recv.at[k], blk=(xs[k]) * NZH + zh
        )
        copy.start()
        copies.append(copy)

    norm = jnp.zeros((1, LANES), F32)
    for q in range(count):
        mine = jnp.concatenate(
            [
                jnp.where(lane == 0, held[q] if g == 0 else pltpu.roll(held[q], LANES - SLOT * g, 1), 0.0)
                for g in range(4)
            ],
            axis=0,
        )
        high = mine.astype(BF16).astype(F32)
        both = (high + pltpu.roll(mine - high, SLOT, 1)).astype(BF16)
        for tile in range(tiles):
            near = both[band[tile] : band[tile] + LANES]
            mixed = nn(gram_hi[q, tile], near) + nn(gram_lo[q, tile], near)
            mixed += pltpu.roll(mixed, LANES - SLOT, 1)
            own_at = tile * BAND
            each = jnp.sum(mixed * mine[own_at : own_at + BAND], axis=1, keepdims=True)
            norm += jnp.sum(member[own_at : own_at + BAND] * each, axis=0, keepdims=True)

    plane[pp] = norm

    for k in range(NX):
        for j in range(NY):
            for i in range(NC):
                if k or j or i:
                    remote(
                        plane.at[pp],
                        plane.at[pp],
                        plane_send,
                        plane_recv,
                        dp=dp_of(zl, ys[j], cs[i]),
                        blk=xs[k] * NZH + zh,
                    ).start()

    for copy in copies:
        copy.wait_recv()
    sends += copies
    pieces = []
    for g in range(4):
        piece = jnp.zeros((tokens // 4, LANES), F32)
        for q in range(4):
            packed = proj[q // count, q % count]
            if g != q:
                packed = pltpu.roll(packed, SLOT * (q - g) % LANES, 1)
            piece = jnp.where(lane == q, packed, piece)
        pieces.append(piece)
    high, low = split(jnp.concatenate(pieces, axis=0))
    eye = (
        lax.broadcasted_iota(jnp.int32, (LANES, LANES), 0)
        == lax.broadcasted_iota(jnp.int32, (LANES, LANES), 1)
    ).astype(F32).astype(BF16)
    high_t, low_t = nt(eye, high), nt(eye, low)
    for e in range(EX):
        here = jnp.broadcast_to(ids_ref[...], (SLOT, tokens)) == e
        for i in range(4):
            at = SLOT * PAIR[i]
            for n, part_t in enumerate((high_t, low_t)):
                left[i, (2 * e + n) * SLOT : (2 * e + n + 1) * SLOT] = jnp.where(
                    here, part_t[at : at + SLOT], 0.0
                ).astype(BF16)

    reached = reach // 72
    cut = reached * 2 * SLOT

    def examples_of(arrays):
        for i in arrays:
            step = 256 if widths[i] % 256 == 0 else LANES
            for k in range(0, widths[i], step):
                across = slice(offsets[i] + k, offsets[i] + k + step)
                early = nn(left[i, :cut, :reach], wide[:reach, across])
                early = early.reshape(reached, 2, SLOT // 8, 8, step)
                singles[:reached, :, :, across] = early[:, 0] + early[:, 1]
                later = nn(left[i, cut:], wide[:, across])
                later = later.reshape(EX - reached, 2, SLOT // 8, 8, step)
                singles[reached:, :, :, across] = later[:, 0] + later[:, 1]

    examples_of((0, 3))

    rest = plane.at[pl.ds(0, npl - 1)]
    remote(rest, rest, plane_send, plane_recv, dp=dp_of(zl, y, 1 - c)).wait()
    everyone = jnp.sum(plane[...], axis=0)
    group = jnp.zeros((1, LANES), F32)
    for k in range(NX):
        group += plane[(k * NY + y) * NC + c]
    ring[zz] = jnp.concatenate([group, everyone], axis=0)

    for k in sorted(range(NZH), key=lambda d: -min(d, NZH - d)):
        for j in range(NZL):
            if k or j:
                remote(
                    ring.at[zz],
                    ring.at[zz],
                    ring_send,
                    ring_recv,
                    dp=dp_of(zls[j], y, c),
                    blk=x * NZH + zhs[k],
                ).start()

    examples_of((1, 2))

    rest = ring.at[pl.ds(0, nz - 1)]
    remote(rest, rest, ring_send, ring_recv, dp=dp_of(zl, y, 1 - c)).wait()
    everyone = jnp.sum(ring[...], axis=0)[1:2]
    group = jnp.zeros((1, LANES), F32)
    for k in range(NZH):
        group += ring[k * NZL + zl][0:1]
    grand_total = jnp.sum(everyone, axis=1, keepdims=True)
    root_mean = jnp.sqrt(jnp.maximum(grand_total, 0.0) / (ranks * EX) + 1e-06)
    clip = (0.5 + 0.125 * thr_ref[...].astype(F32)) * root_mean
    factor = jnp.minimum(1.0, clip * lax.rsqrt(jnp.maximum(group, 0.0) + 1e-06))
    entries = 2 * ranks * NX * NZH * (widths[0] + widths[1])
    rescale = math.sqrt(entries / (ranks * EX)) / clip
    scaled = factor * rescale
    lane = lax.broadcasted_iota(jnp.int32, (1, LANES), 1)
    weights = [
        jnp.broadcast_to(
            jnp.sum(jnp.where(lane == e, scaled, 0.0), axis=1, keepdims=True), (8, LANES)
        )
        for e in range(EX)
    ]

    def clipped(g):
        for i in range(4):
            for j in range(chunks[i]):
                at = offsets[i] + j * LANES
                total = weights[0] * singles[0, g, :, at : at + LANES]
                for e in range(1, EX):
                    total += weights[e] * singles[e, g, :, at : at + LANES]
                grads[pl.ds(g * (8 * block) + firsts[i] + j, 8, stride=block), :] = total

    wide_block = NY * block
    groups = NZL * NY // 8
    if groups == 2:
        pair_at = zl // 2
        away = 2 * lax.rem(pair_at + 1, 2)
        other = 2 * pair_at + 1 - lax.rem(zl, 2)
        order = [away, away + 1, other, zl]
        sets = [lax.rem(pair_at + 1, 2), pair_at]
    else:
        order = [1 - zl, zl]
        sets = [0] * groups
        if not groups:
            for g in range(-(-ranks // 8)):
                clipped(g)
    batch = len(order) // max(groups, 1)
    copies = []
    for n in range(max(groups, 1)):
        if groups:
            clipped((1 - c) * groups + sets[n])
        for o in range(n * batch, (n + 1) * batch):
            at = pl.multiple_of(((1 - c) * NZL + order[o]) * wide_block, 8)
            copy = remote(
                grads.at[pl.ds(at, wide_block)],
                pair_in.at[o],
                pair_send.at[o],
                pair_recv.at[o],
                dp=dp_of(zl, y, 1 - c),
            )
            copy.start()
            copies.append(copy)
    sends += copies
    y_copies = {}
    for n in range(max(groups, 1)):
        if groups:
            clipped(c * groups + sets[n])
        for o in range(n * batch, (n + 1) * batch):
            at = pl.multiple_of((c * NZL + order[o]) * wide_block, 8)
            copies[o].wait_recv()
            pair_sum[o] = (grads[pl.ds(at, wide_block), :] + pair_in[o]).reshape(NY, block, LANES)
            for j in range(1, NY):
                copy = remote(
                    pair_sum.at[o, ys[j]],
                    y_in.at[o, y],
                    y_send.at[o, j],
                    y_recv.at[o, j],
                    dp=dp_of(zl, ys[j], c),
                )
                copy.start()
                y_copies[o, j] = copy
    last = NZL - 1
    for o in range(NZL):
        held = pair_sum[o, y]
        for j in range(1, NY):
            y_copies[o, j].wait_recv()
            sends.append(y_copies[o, j])
        for j in range(1, NY):
            held += y_in[o, ys[j]]
        if o < last:
            z_out[o] = held
            copy = remote(
                z_out.at[o], z_in.at[zl], z_send.at[o], z_recv.at[zl], dp=dp_of(order[o], y, c)
            )
            copy.start()
            sends.append(copy)
    for k in range(1, NZL):
        remote(
            z_in.at[zls[k]], z_in.at[zls[k]], z_send.at[0], z_recv.at[zls[k]], dp=dp_of(zl, y, 1 - c)
        ).wait_recv()
    for k in range(1, NZL):
        held += z_in[zls[k]]
    row_f32[: held.shape[0], :] = held
    at = 0
    for ref in (model_out, hidden_out):
        for k in range(2):
            for j in range(ref.shape[2] // LANES):
                ref[k, :, j * LANES : (j + 1) * LANES] = row_f32[at : at + 1, :]
                at += 1
    for copy in sends:
        copy.wait_send()


def per_device(
    block_input_rows,
    up_loss_gradient,
    down_projection_input,
    output_loss_gradient,
    model_side_factors,
    hidden_side_factors,
    example_index_rows,
    clipping_threshold,
    model_side_noise,
    hidden_side_noise,
):
    ndp, nblk = lax.axis_size("dp"), lax.axis_size("blk")
    NZL, NY, NC = DP_AXES[ndp]
    NX, NZH = BLK_AXES[nblk]
    tokens = block_input_rows.shape[0]
    model, hidden = block_input_rows.shape[1], up_loss_gradient.shape[1]
    widths = (model, hidden, hidden, model)
    total = sum(widths)
    rows = total // LANES
    block = -(-rows // 8) * 8
    sent = -(-rows // 16) * 16
    cfg = (NZL, NY, NC, NX, NZH, widths, block)
    count, tiles = 4 // NX, tokens // BAND
    dma = pltpu.SemaphoreType.DMA
    vmem = pl.BlockSpec(memory_space=pltpu.VMEM)
    hbm = pl.BlockSpec(memory_space=pl.ANY)
    summed = pl.pallas_call(
        functools.partial(kernel, cfg),
        out_shape=[
            jax.ShapeDtypeStruct(model_side_noise.shape, F32),
            jax.ShapeDtypeStruct(hidden_side_noise.shape, F32),
        ],
        in_specs=[vmem, vmem, vmem, vmem, hbm, hbm, hbm, hbm],
        out_specs=[vmem, vmem],
        scratch_shapes=[
            pltpu.VMEM((tokens, total), BF16),
            pltpu.VMEM((sent, LANES), F32),
            pltpu.VMEM((sent, LANES), BF16),
            pltpu.VMEM((ndp, sent, LANES), BF16),
            pltpu.VMEM((ndp * block, LANES), F32),
            pltpu.VMEM((LANES, total), BF16),
            pltpu.VMEM((NX, count, tiles, BAND, LANES), F32),
            pltpu.VMEM((NX, count, tiles, BAND, LANES), F32),
            pltpu.VMEM((count, tiles, BAND, LANES), BF16),
            pltpu.VMEM((count, tiles, BAND, LANES), BF16),
            pltpu.VMEM((NX, count, tokens // 4, LANES), F32),
            pltpu.VMEM((NX, count, tokens // 4, LANES), F32),
            pltpu.VMEM((count, tokens // 4, LANES), F32),
            pltpu.VMEM((NZH, count, tokens // 4, LANES), F32),
            pltpu.VMEM((NX, count, tokens // 4, LANES), F32),
            pltpu.VMEM((NX * NY * NC, 1, LANES), F32),
            pltpu.VMEM((NZL * NZH, 2, LANES), F32),
            pltpu.VMEM((4, 2 * EX * SLOT, tokens), BF16),
            pltpu.VMEM((EX, SLOT // 8, 8, total), F32),
            pltpu.VMEM((ndp * block, LANES), F32),
            pltpu.VMEM((NZL, NY * block, LANES), F32),
            pltpu.VMEM((NZL, NY, block, LANES), F32),
            pltpu.VMEM((NZL, NY, block, LANES), F32),
            pltpu.VMEM((NZL, block, LANES), F32),
            pltpu.VMEM((NZL, block, LANES), F32),
            dma((4,)),
            dma((ndp,)),
            dma((ndp,)),
            dma((NX,)),
            dma((NX,)),
            dma((NX,)),
            dma((NX,)),
            dma((NZH,)),
            dma((NZH,)),
            dma((NX,)),
            dma((NX,)),
            dma,
            dma,
            dma,
            dma,
            dma((NZL,)),
            dma((NZL,)),
            dma((NZL, NY)),
            dma((NZL, NY)),
            dma((NZL,)),
            dma((NZL,)),
            pltpu.SemaphoreType.REGULAR((2,)),
        ],
        compiler_params=pltpu.CompilerParams(
            collective_id=0, has_side_effects=True, vmem_limit_bytes=56 << 20
        ),
        name="clipped_step",
    )(
        clipping_threshold.reshape(1, 1),
        example_index_rows,
        model_side_factors.reshape(2, model),
        hidden_side_factors.reshape(2, hidden),
        block_input_rows,
        up_loss_gradient,
        down_projection_input,
        output_loss_gradient,
    )
    return (summed[0] + model_side_noise, summed[1] + hidden_side_noise)


def solution(mesh):
    in_specs = (
        P("dp", "blk"),
        P("dp", "blk"),
        P("dp", "blk"),
        P("dp", "blk"),
        P(None, "dp", "blk"),
        P(None, "dp", "blk"),
        P("dp", None),
        P(),
        P(None, "dp", "blk"),
        P(None, "dp", "blk"),
    )
    out_specs = (P(None, "dp", "blk"), P(None, "dp", "blk"))
    return jax.shard_map(
        per_device,
        mesh=mesh,
        in_specs=in_specs,
        out_specs=out_specs,
        check_vma=False,
    )
```
